32 devices in a mesh: dp: 2 (over z, core), sp: 16 (over x, y).
Axes of the slice: x: 4, y: 4, z: 1, core: 2. Of those that a mesh axis runs over, the one named last changes fastest.
The devices are a block of a 4x4x8 slice.
Arguments:
- x: bfloat16 [8192, 4608], P(('dp', 'sp')), parts along dimension 0
- gain: bfloat16 [4608], replicated
- wq: bfloat16 [4608, 4096], replicated
- wk: bfloat16 [4608, 2048], replicated
- wv: bfloat16 [4608, 2048], replicated
- wo: bfloat16 [4096, 4608], replicated
Outputs:
- output: bfloat16 [8192, 4608], P(('dp', 'sp')), parts along dimension 0
There are 2 independent parts. The reference program is written for one: setup_inputs(seed, part) draws one part's arguments, and reference() takes and returns one part's arrays. A program takes and returns all parts, laid end to end along the dimension named above; an argument that names none is the same for every part.
All inputs are finite; a program needn't handle non-finite values.
Results may differ from the reference program's by a relative error of at most 0.012.
Values are sent between devices in bfloat16 or wider.
A program may use at most 768 MiB of HBM per device.

```python
import jax
import jax.numpy as jnp
from jax import lax

ROWS = 4096
D = 4608
HEADS = 32
KV_HEADS = 16
HEAD = 128
THETA = 10000


def setup_inputs(seed: int = 0, part: int = 0) -> dict:
    kx, kn, kq, kk, kv, ko = jax.random.split(jax.random.key(seed), 6)

    def weights(key, rows, columns):
        return jax.random.normal(key, (rows, columns), jnp.float32) * rows**-0.5

    drawn = {
        "x": jax.random.normal(jax.random.fold_in(kx, part), (ROWS, D), jnp.float32),
        "gain": 1 + 0.1 * jax.random.normal(kn, (D,), jnp.float32),
        "wq": 2 * weights(kq, D, HEADS * HEAD),
        "wk": 2 * weights(kk, D, KV_HEADS * HEAD),
        "wv": 4 * weights(kv, D, KV_HEADS * HEAD),
        "wo": weights(ko, HEADS * HEAD, D),
    }
    return {k: v.astype(jnp.bfloat16) for k, v in drawn.items()}


def normed(x, gain):
    wide = x.astype(jnp.float32)
    scale = lax.rsqrt(jnp.mean(wide * wide, -1, keepdims=True) + 1e-6)
    return (wide * scale * gain.astype(jnp.float32)).astype(jnp.bfloat16)


def turned(t, place, theta):
    half = t.shape[-1] // 2
    angle = place.astype(jnp.float32)[:, None] * theta ** (-jnp.arange(half, dtype=jnp.float32) / half)
    cos, sin = jnp.cos(angle)[:, None], jnp.sin(angle)[:, None]
    a, b = t[..., :half].astype(jnp.float32), t[..., half:].astype(jnp.float32)
    return jnp.concatenate([a * cos - b * sin, b * cos + a * sin], -1).astype(jnp.bfloat16)


def matmul(a, w):
    return jnp.dot(a, w, preferred_element_type=jnp.float32).astype(jnp.bfloat16)


def einsum(form, a, b):
    return jnp.einsum(form, a.astype(jnp.float32), b.astype(jnp.float32))


def attention(q, k, v):
    scores = einsum("tgsd,ugd->gstu", q, k) * q.shape[-1] ** -0.5
    token = jnp.arange(q.shape[0])
    scores = jnp.where(token[:, None] >= token, scores, -jnp.inf)
    weights = jax.nn.softmax(scores, -1).astype(jnp.bfloat16)
    return einsum("gstu,ugd->tgsd", weights, v).astype(jnp.bfloat16)


def reference(x, gain, wq, wk, wv, wo):
    a, place = normed(x, gain), jnp.arange(ROWS)
    q = turned(matmul(a, wq).reshape(ROWS, HEADS, HEAD), place, THETA).reshape(ROWS, KV_HEADS, -1, HEAD)
    k = turned(matmul(a, wk).reshape(ROWS, KV_HEADS, HEAD), place, THETA)
    v = matmul(a, wv).reshape(ROWS, KV_HEADS, HEAD)
    seen = attention(q, k, v).reshape(ROWS, HEADS * HEAD)
    return (x.astype(jnp.float32) + jnp.dot(seen, wo, preferred_element_type=jnp.float32)).astype(jnp.bfloat16)
```

```python
import functools

import jax
import jax.numpy as jnp
from jax import lax
from jax.experimental import pallas as pl
from jax.experimental.pallas import tpu as pltpu
from jax.sharding import PartitionSpec as P

HEAD = 128
THETA = 10000
NEG = -1e30
HIDDEN = 2 * NEG
LOG2E = 1.4426950408889634
COLS = 512
ONES = 16
WO_SLOTS = 6


def _dot(a, b, ca=1, cb=0):
    return lax.dot_general(a, b, (((ca,), (cb,)), ((), ())), preferred_element_type=jnp.float32)


def _kernel(n, x_hbm, gain_ref, cos_ref, sin_ref, wq, wk, wv, wo, y_hbm,
            xv, av, wbuf, wobuf, ksend, vsend, qsend, kbuf, vbuf, qbuf, osend, obuf, acc, top_s, mix_s,
            xsem, wsem, wosem, ss, rs):
    me = lax.axis_index("sp")
    own, dim = xv.shape
    slots = wbuf.shape[0]
    qc, kc = qsend.shape[1] // own * HEAD, HEAD
    q_chunks, k_chunks = wq.shape[1] // COLS, wk.shape[1] // COLS
    q_per, k_per = COLS // qc, COLS // kc
    g = qc // HEAD
    cols = g * own

    def chunk(w, c, chunks, per, slot):
        at = lax.rem(lax.div(me, per) + c, chunks)
        return at, pltpu.make_async_copy(w.at[:, pl.ds(at * COLS, COLS)], wbuf.at[slot], wsem.at[slot])

    k_chunk = lambda c: chunk(wk, c, k_chunks, k_per, c)
    v_chunk = lambda c: chunk(wv, c, k_chunks, k_per, c)
    q_chunk = lambda c: chunk(wq, c, q_chunks, q_per, lax.rem(c, slots))

    get_x = pltpu.make_async_copy(x_hbm, xv, xsem.at[0])
    get_x.start()
    for c in range(slots):
        k_chunk(c)[1].start()

    barrier = pltpu.get_barrier_semaphore()

    def greet(s, _):
        pl.semaphore_signal(barrier, inc=1, device_id={"sp": lax.rem(me + s, n)})

    lax.fori_loop(1, n, greet, None)

    get_x.wait()
    strip = 32
    gain = gain_ref[...].astype(jnp.float32)

    def norm(i, _):
        rows = pl.ds(pl.multiple_of(i * strip, strip), strip)
        wide = xv[rows, :].astype(jnp.float32)
        scale = lax.rsqrt(jnp.mean(wide * wide, -1, keepdims=True) + 1e-6)
        av[rows, :] = (wide * scale * gain).astype(jnp.bfloat16)

    lax.fori_loop(0, own // strip, norm, None)
    for b in range(n):
        vbuf[b, HEAD:, :] = jnp.ones((ONES, own), jnp.bfloat16)
    pl.semaphore_wait(barrier, n - 1)

    def remote(kind, src, dst, to):
        return pltpu.make_async_remote_copy(src_ref=src.at[to], dst_ref=dst.at[me], send_sem=ss.at[kind, to], recv_sem=rs.at[kind, me],
                                            device_id={"sp": to})

    def local(kind, src, dst):
        return pltpu.make_async_copy(src.at[me], dst.at[me], rs.at[kind, me])

    def send(kind, src, dst, to):
        @pl.when(to != me)
        def _():
            remote(kind, src, dst, to).start()

        @pl.when(to == me)
        def _():
            local(kind, src, dst).start()

    def arrived(kind, dst, at):
        pltpu.make_async_copy(dst.at[at], dst.at[at], rs.at[kind, at]).wait()

    def sent(kind, src, s):
        to = lax.rem(me + s, n)
        pltpu.make_async_copy(src.at[to], src.at[to], ss.at[kind, to]).wait()

    vdst = vbuf.at[:, pl.ds(0, HEAD), :]

    def turned(t):
        t = t.astype(jnp.bfloat16).astype(jnp.float32)
        return (t * cos_ref[...] + pltpu.roll(t, HEAD // 2, 1) * sin_ref[...]).astype(jnp.bfloat16)

    def keys(c, _):
        at, get = k_chunk(c)
        get.wait()
        r = _dot(av[...], wbuf[c])
        v_chunk(c)[1].start()
        for i in range(k_per):
            ksend[at * k_per + i] = turned(r[:, i * HEAD:(i + 1) * HEAD])
        for i in range(k_per):
            send(0, ksend, kbuf, at * k_per + i)

    lax.fori_loop(0, k_chunks, keys, None)

    def values(c, _):
        at, get = v_chunk(c)
        get.wait()
        r = _dot(av[...], wbuf[c])
        q_chunk(c)[1].start()
        for i in range(k_per):
            vsend[at * k_per + i] = r[:, i * HEAD:(i + 1) * HEAD].T.astype(jnp.bfloat16)
        for i in range(k_per):
            send(1, vsend, vdst, at * k_per + i)

    lax.fori_loop(0, k_chunks, values, None)

    def queries(c, _):
        at, get = q_chunk(c)
        get.wait()
        slot = lax.rem(c, slots)
        r = _dot(av[...], wbuf[slot])

        @pl.when(c + slots < q_chunks)
        def _():
            q_chunk(c + slots)[1].start()

        for i in range(q_per):
            for h in range(g):
                qsend[at * q_per + i, h * own:(h + 1) * own, :] = turned(r[:, (i * g + h) * HEAD:(i * g + h + 1) * HEAD])
        for i in range(q_per):
            send(2, qsend, qbuf, at * q_per + i)

    lax.fori_loop(0, q_chunks, queries, None)

    def wo_rows(s):
        src = lax.rem(me + s, n)
        slot = lax.rem(s, WO_SLOTS)
        return pltpu.make_async_copy(wo.at[pl.ds(src * qc, qc), :], wobuf.at[slot], wosem.at[slot])

    for s in range(WO_SLOTS):
        wo_rows(s).start()

    def all_kv(s, _):
        at = lax.rem(me + n - s, n)
        arrived(0, kbuf, at)
        arrived(1, vdst, at)

    lax.fori_loop(0, n, all_kv, None)
    e = HEAD**-0.5 * LOG2E

    def attend(s, _):
        b = lax.rem(me + n - s, n)
        arrived(2, qbuf, b)
        top_s[...] = jnp.full(top_s.shape, NEG, jnp.float32)
        mix_s[...] = jnp.zeros(mix_s.shape, jnp.float32)
        whole = lax.div(b, 2)

        def block(j, masked):
            k = kbuf[pl.ds(2 * j, 2)].reshape(2 * own, HEAD)
            scores = [_dot(k, qbuf[b, h * own:(h + 1) * own, :], 1, 1) for h in range(g)]
            if masked:
                gap = lax.broadcasted_iota(jnp.int32, (2 * own, own), 1) - lax.broadcasted_iota(jnp.int32, (2 * own, own), 0)
                ok = gap >= (2 * j - b) * own
            weights, keeps = [], []
            for h, sc in enumerate(scores):
                here = slice(h * own, (h + 1) * own)
                if masked:
                    sc = jnp.where(ok, sc, HIDDEN)
                old = top_s[0:1, here]
                top = jnp.maximum(old, sc.max(axis=0, keepdims=True))
                top_s[0:1, here] = top
                weights.append(jnp.exp2((sc - top) * e).astype(jnp.bfloat16))
                keeps.append(jnp.exp2((old - top) * e))
            for h in range(g):
                here = slice(h * own, (h + 1) * own)
                new = _dot(vbuf[2 * j], weights[h][:own]) + _dot(vbuf[2 * j + 1], weights[h][own:])
                mix_s[:, here] = mix_s[:, here] * keeps[h] + new

        lax.fori_loop(0, whole, lambda j, _: block(j, False), None)
        block(whole, True)
        for h in range(g):
            here = slice(h * own, (h + 1) * own)
            out = mix_s[:HEAD, here] * (1 / mix_s[HEAD:HEAD + 1, here])
            osend[b, :, h * HEAD:(h + 1) * HEAD] = out.T.astype(jnp.bfloat16)
        send(3, osend, obuf, b)

    lax.fori_loop(0, n, attend, None)

    acc[...] = xv[...].astype(jnp.float32)
    half = COLS

    def project(i, _):
        pair = []
        for s in (2 * i, 2 * i + 1):
            src = lax.rem(me + s, n)
            arrived(3, obuf, src)
            wo_rows(s).wait()
            pair.append((src, lax.rem(s, WO_SLOTS)))
        for at in range(0, dim, half):
            new = sum(_dot(obuf[src], wobuf[slot, :, at:at + half]) for src, slot in pair)
            acc[:, at:at + half] = acc[:, at:at + half] + new
        for s in (2 * i, 2 * i + 1):
            @pl.when(s + WO_SLOTS < n)
            def _():
                wo_rows(s + WO_SLOTS).start()

    lax.fori_loop(0, n // 2, project, None)
    av[...] = acc[...].astype(jnp.bfloat16)
    put = pltpu.make_async_copy(av, y_hbm, xsem.at[0])
    put.start()

    def drain(s, _):
        sent(0, ksend, s)
        sent(1, vsend, s)
        sent(2, qsend, s)
        sent(3, osend, s)

    lax.fori_loop(1, n, drain, None)
    put.wait()


def solution(mesh):
    n = mesh.shape["sp"]

    def step(x, gain, wq, wk, wv, wo):
        own, dim = x.shape
        qc, kc = wq.shape[1] // n, wk.shape[1] // n
        g = qc // HEAD
        half = HEAD // 2
        place = lax.axis_index("sp") * own + jnp.arange(own)
        angle = place.astype(jnp.float32)[:, None] * THETA ** (-jnp.arange(half, dtype=jnp.float32) / half)
        cos, sin = jnp.cos(angle), jnp.sin(angle)
        cos, sin = jnp.concatenate([cos, cos], -1), jnp.concatenate([-sin, sin], -1)
        low = jnp.bfloat16
        anywhere, vmem = pl.BlockSpec(memory_space=pl.ANY), pl.BlockSpec(memory_space=pltpu.VMEM)
        return pl.pallas_call(
            functools.partial(_kernel, n),
            out_shape=jax.ShapeDtypeStruct((own, dim), low),
            in_specs=[anywhere, vmem, vmem, vmem, anywhere, anywhere, anywhere, anywhere],
            out_specs=anywhere,
            scratch_shapes=[
                pltpu.VMEM((own, dim), low),
                pltpu.VMEM((own, dim), low),
                pltpu.VMEM((wk.shape[1] // COLS, dim, COLS), low),
                pltpu.VMEM((WO_SLOTS, qc, dim), low),
                pltpu.VMEM((n, own, HEAD), low),
                pltpu.VMEM((n, HEAD, own), low),
                pltpu.VMEM((n, g * own, HEAD), low),
                pltpu.VMEM((n, own, HEAD), low),
                pltpu.VMEM((n, HEAD + ONES, own), low),
                pltpu.VMEM((n, g * own, HEAD), low),
                pltpu.VMEM((n, own, qc), low),
                pltpu.VMEM((n, own, qc), low),
                pltpu.VMEM((own, dim), jnp.float32),
                pltpu.VMEM((8, g * own), jnp.float32),
                pltpu.VMEM((HEAD + ONES, g * own), jnp.float32),
                pltpu.SemaphoreType.DMA((1,)),
                pltpu.SemaphoreType.DMA((wk.shape[1] // COLS,)),
                pltpu.SemaphoreType.DMA((WO_SLOTS,)),
                pltpu.SemaphoreType.DMA((4, n)),
                pltpu.SemaphoreType.DMA((4, n)),
            ],
            compiler_params=pltpu.CompilerParams(collective_id=0, has_side_effects=True, vmem_limit_bytes=67043328),
        )(x, gain.reshape(1, dim), cos, sin, wq, wk, wv, wo)

    tokens, whole = P(("dp", "sp"), None), P(None, None)
    return jax.shard_map(
        step,
        mesh=mesh,
        in_specs=(tokens, P(None), whole, whole, whole, whole),
        out_specs=tokens,
        check_vma=False,
    )
```

```python
import functools

import jax
import jax.numpy as jnp
from jax import lax
from jax.experimental import pallas as pl
from jax.experimental.pallas import tpu as pltpu
from jax.sharding import PartitionSpec as P

HEAD = 128
THETA = 10000
NEG = -1e30
HIDDEN = 2 * NEG
LOG2E = 1.4426950408889634
COLS = 512
ONES = 16
WO_SLOTS = 4
VMEM = 58 * 2**20


def _dot(a, b, ca=1, cb=0):
    return lax.dot_general(a, b, (((ca,), (cb,)), ((), ())), preferred_element_type=jnp.float32)


def _kernel(n, x_hbm, gain_ref, cos_ref, sin_ref, wq, wk, wv, wo, y_hbm,
            xv, av, wbuf, wobuf, ksend, vsend, qsend, kbuf, vbuf, qbuf, osend, obuf, acc, top_s, mix_s, s0, s1, p0, p1, high0, high1, keep0, keep1, cos_s, sin_s,
            xsem, wsem, wosem, ss, rs):
    me = lax.axis_index("sp")
    s_s, p_s, high_s, keep_s = (s0, s1), (p0, p1), (high0, high1), (keep0, keep1)
    own, dim = xv.shape
    slots = wbuf.shape[0]
    qc, kc = qsend.shape[1] // own * HEAD, HEAD
    q_chunks, k_chunks = wq.shape[1] // COLS, wk.shape[1] // COLS
    q_per, k_per = COLS // qc, COLS // kc
    g = qc // HEAD
    cols = g * own

    side = max(d for d in range(1, n + 1) if n % d == 0 and d * d <= n)
    in_row, down = side // 2, n // side

    def hops(dx, dh, q=None):
        far = [min(2 * dh + i, side - 2 * dh - i) for i in ((0, 1) if q is None else (q,))]
        return min(dx, down - dx) + sum(far) / len(far)

    turns = sorted(((dx, dh) for dh in range(in_row) for dx in range(down)), key=lambda t: (-hops(*t), t[1]))
    kv_turns = sorted(turns, key=lambda t: (-min(t[0], down - t[0]), -t[1]))
    rank = lambda h: h if h < 2 else 2 + max(3 - h, 0)
    meetings = sorted(((*t, q) for t in turns for q in range(2)), key=lambda t: rank(hops(*t)))

    def partner(c, given, sign=1):
        words = [sum((turn[0] | turn[1] << 3 | (turn[2] if len(turn) > 2 else 0) << 6) << (7 * i) for i, turn in enumerate(given[a:a + 4]))
                 for a in range(0, len(given), 4)]
        word = functools.reduce(lambda low, a: jnp.where(c >= 4 * a, words[a], low), range(1, len(words)), words[0])
        code = lax.shift_right_logical(word, 7 * lax.rem(c, 4))
        row = lax.rem(my_row + down + sign * (code & 7), down)
        return 2 * (row * in_row + lax.rem(my_place + in_row + sign * (lax.shift_right_logical(code, 3) & 7), in_row)), lax.shift_right_logical(code, 6) & 1

    my_row, my_place = lax.div(me, side), lax.div(lax.rem(me, side), 2)

    def meet(s, sign):
        pair, q = partner(s, meetings, sign)
        return pair + lax.rem(me + q, 2)

    asker = lambda s: meet(s, -1)
    answerer = lambda s: meet(s, 1)

    def kv_pairs(c):
        return [partner(2 * c + i, kv_turns)[0] for i in range(2)]

    def kv_chunk(w, c):
        wide = 2 * kc
        return [pltpu.make_async_copy(w.at[:, pl.ds(p * kc, wide)], wbuf.at[c, :, pl.ds(i * wide, wide)], wsem.at[c])
                for i, p in enumerate(kv_pairs(c))]

    def q_chunk(c):
        at, slot = partner(c, turns)[0], lax.rem(c, slots)
        return [pltpu.make_async_copy(wq.at[:, pl.ds(at * qc, COLS)], wbuf.at[slot], wsem.at[slot])]

    def start(given):
        for copy in given:
            copy.start()

    def filled(slot):
        pltpu.make_async_copy(wbuf.at[slot], wbuf.at[slot], wsem.at[slot]).wait()

    get_x = pltpu.make_async_copy(x_hbm, xv, xsem.at[0])
    get_x.start()

    barrier = pltpu.get_barrier_semaphore()

    def greet(s, _):
        pl.semaphore_signal(barrier, inc=1, device_id={"sp": lax.rem(me + s, n)})

    lax.fori_loop(1, n, greet, None)

    start(kv_chunk(wk, 0))
    cos_s[...] = jnp.concatenate([cos_ref[...], cos_ref[...]], axis=1)
    sin_s[...] = jnp.concatenate([-sin_ref[...], sin_ref[...]], axis=1)

    get_x.wait()
    for c in range(1, slots):
        start(kv_chunk(wk, c))
    strip = 32
    gain = gain_ref[...].astype(jnp.float32)
    lanes = gain.shape[1]

    def norm(i, _):
        rows = pl.ds(pl.multiple_of(i * strip, strip), strip)
        wide = xv[rows, :].astype(jnp.float32)
        scale = lax.rsqrt(jnp.mean(wide * wide, -1, keepdims=True) + 1e-6)
        for c in range(dim // lanes):
            here = slice(c * lanes, (c + 1) * lanes)
            av[rows, here] = (wide[:, here] * scale * gain[c:c + 1, :]).astype(jnp.bfloat16)

    lax.fori_loop(0, own // strip, norm, None)
    for b in range(n):
        vbuf[b, HEAD:, :] = jnp.ones((ONES, own), jnp.bfloat16)

    def remote(kind, src, dst, to):
        return pltpu.make_async_remote_copy(src_ref=src.at[to], dst_ref=dst.at[me], send_sem=ss.at[kind, to], recv_sem=rs.at[kind, me],
                                            device_id={"sp": to})

    def local(kind, src, dst):
        return pltpu.make_async_copy(src.at[me], dst.at[me], rs.at[kind, me])

    def send(kind, src, dst, to):
        @pl.when(to != me)
        def _():
            remote(kind, src, dst, to).start()

        @pl.when(to == me)
        def _():
            local(kind, src, dst).start()

    def arrived(kind, dst, at):
        pltpu.make_async_copy(dst.at[at], dst.at[at], rs.at[kind, at]).wait()

    def sent(kind, src, s):
        to = lax.rem(me + s, n)
        pltpu.make_async_copy(src.at[to], src.at[to], ss.at[kind, to]).wait()

    vdst = vbuf.at[:, pl.ds(0, HEAD), :]

    def turned(t):
        t = t.astype(jnp.bfloat16).astype(jnp.float32)
        return (t * cos_s[...] + pltpu.roll(t, HEAD // 2, 1) * sin_s[...]).astype(jnp.bfloat16)

    def keys(c, _):
        at = kv_pairs(c)
        filled(c)
        r = _dot(av[...], wbuf[c])
        start(kv_chunk(wv, c))
        for i in range(k_per):
            ksend[at[i // 2] + i % 2] = turned(r[:, i * HEAD:(i + 1) * HEAD])

        @pl.when(c == 0)
        def _():
            pl.semaphore_wait(barrier, n - 1)

        for i in range(k_per):
            send(0, ksend, kbuf, at[i // 2] + i % 2)

    lax.fori_loop(0, k_chunks, keys, None)

    def values(c, _):
        at = kv_pairs(c)
        filled(c)
        r = _dot(av[...], wbuf[c])
        start(q_chunk(c))
        for i in range(k_per):
            vsend[at[i // 2] + i % 2] = r[:, i * HEAD:(i + 1) * HEAD].T.astype(jnp.bfloat16)
        for i in range(k_per):
            send(1, vsend, vdst, at[i // 2] + i % 2)

    lax.fori_loop(0, k_chunks, values, None)

    def queries(c, _):
        at, slot = partner(c, turns)[0], lax.rem(c, slots)
        filled(slot)
        r = _dot(av[...], wbuf[slot])

        @pl.when(c + slots < q_chunks)
        def _():
            start(q_chunk(c + slots))

        for i in range(q_per):
            for h in range(g):
                qsend[at + i, h * own:(h + 1) * own, :] = turned(r[:, (i * g + h) * HEAD:(i * g + h + 1) * HEAD])
    lax.fori_loop(0, q_chunks, queries, None)
    lax.fori_loop(0, n, lambda s, _: send(2, qsend, qbuf, answerer(s)), None)

    def wo_rows(s):
        src = answerer(s)
        slot = lax.rem(s, WO_SLOTS)
        return pltpu.make_async_copy(wo.at[pl.ds(src * qc, qc), :], wobuf.at[slot], wosem.at[slot])

    for s in range(WO_SLOTS):
        wo_rows(s).start()

    e = HEAD**-0.5 * LOG2E

    def following(s, b, j):
        last = j == lax.div(b, 2)
        s = jnp.where(last, s + 1, s)
        return s, asker(s), jnp.where(last, 0, j + 1)

    heads = [slice(h * own, (h + 1) * own) for h in range(g)]

    def scores(slot, b, j, masked):
        k = kbuf[pl.ds(2 * j, 2)].reshape(2 * own, HEAD)
        for here in heads:
            sc = _dot(k, qbuf[b, here, :], 1, 1)
            if masked:
                gap = lax.broadcasted_iota(jnp.int32, (2 * own, own), 1) - lax.broadcasted_iota(jnp.int32, (2 * own, own), 0)
                sc = jnp.where(gap >= (2 * j - b) * own, sc, HIDDEN)
            s_s[slot][:, here] = sc
            high_s[slot][0:1, here] = sc.max(axis=0, keepdims=True)

    def weights(slot, j, h):
        here = heads[h]
        old = jnp.where(j == 0, NEG, top_s[0:1, here])
        top = jnp.maximum(old, high_s[slot][0:1, here])
        top_s[0:1, here] = top
        keep_s[slot][0:1, here] = jnp.exp2((old - top) * e)
        p_s[slot][:, here] = jnp.exp2((s_s[slot][:, here] - top) * e).astype(jnp.bfloat16)

    def mix(slot, j, h):
        here = heads[h]
        new = _dot(vbuf[2 * j], p_s[slot][:own, here]) + _dot(vbuf[2 * j + 1], p_s[slot][own:, here])
        mix_s[:, here] = mix_s[:, here] * keep_s[slot][0:1, here] + new

    def finish(b, h):
        here = heads[h]
        out = mix_s[:HEAD, here] * (1 / mix_s[HEAD:HEAD + 1, here])
        osend[b, :, h * HEAD:(h + 1) * HEAD] = out.T.astype(jnp.bfloat16)

    def keys_of(j, _=None):
        for at in (2 * j, 2 * j + 1):
            arrived(0, kbuf, at)
            arrived(1, vdst, at)

    def ready(b, j, seen):
        @pl.when(j == 0)
        def _():
            arrived(2, qbuf, b)

        @pl.when(j > seen)
        def _():
            keys_of(j)

        return jnp.maximum(seen, j)

    def pair(i, at, final=False):
        (s0, b0, j0), (b1, j1), seen = at
        for slot in range(2):
            s2, b2, j2 = following(s0, b0, j0)
            if not final or slot == 0:
                seen = ready(b2, j2, seen)
            for masked in (False, True):
                @pl.when((j2 == lax.div(b2, 2)) == masked)
                def _():
                    if not final or slot == 0:
                        scores(1 - slot, b2, j2, masked)
                    weights(slot, j0, 0)
                    mix(slot, j0, 0)
                    weights(slot, j0, 1)
                    mix(1 - slot, j1, 1)

            @pl.when((j1 == lax.div(b1, 2)) & (i + slot > 0))
            def _():
                finish(b1, 1)
                send(3, osend, obuf, b1)

            @pl.when(j0 == lax.div(b0, 2))
            def _():
                finish(b0, 0)

            (s0, b0, j0), (b1, j1) = (s2, b2, j2), (b0, j0)
        return (s0, b0, j0), (b1, j1), seen

    steps = sum(b // 2 + 1 for b in range(n))
    p_s[1][...] = jnp.zeros(p_s[1].shape, jnp.bfloat16)
    keep_s[1][...] = jnp.zeros(keep_s[1].shape, jnp.float32)
    mix_s[...] = jnp.zeros(mix_s.shape, jnp.float32)
    zero = me - me
    ready(me, zero, zero - 1)
    for masked in (False, True):
        @pl.when((lax.div(me, 2) == 0) == masked)
        def _():
            scores(0, me, 0, masked)
    at = lax.fori_loop(0, steps // 2 - 1, pair, ((zero, me, zero), (me, zero), zero))
    at = pair(1, at, True)
    mix(1, at[1][1], 1)
    finish(at[1][0], 1)
    send(3, osend, obuf, at[1][0])

    acc[...] = xv[...].astype(jnp.float32)
    half = COLS

    def project(i, _):
        pair = []
        for s in (2 * i, 2 * i + 1):
            src = answerer(s)
            arrived(3, obuf, src)
            wo_rows(s).wait()
            pair.append((src, lax.rem(s, WO_SLOTS)))
        for at in range(0, dim, half):
            new = sum(_dot(obuf[src], wobuf[slot, :, at:at + half]) for src, slot in pair)
            acc[:, at:at + half] = acc[:, at:at + half] + new
        for s in (2 * i, 2 * i + 1):
            @pl.when(s + WO_SLOTS < n)
            def _():
                wo_rows(s + WO_SLOTS).start()

    lax.fori_loop(0, n // 2, project, None)
    av[...] = acc[...].astype(jnp.bfloat16)
    put = pltpu.make_async_copy(av, y_hbm, xsem.at[0])
    put.start()

    def drain(s, _):
        sent(0, ksend, s)
        sent(1, vsend, s)
        sent(2, qsend, s)
        sent(3, osend, s)

    lax.fori_loop(1, n, drain, None)
    put.wait()


def solution(mesh):
    n = mesh.shape["sp"]

    def step(x, gain, wq, wk, wv, wo):
        own, dim = x.shape
        qc, kc = wq.shape[1] // n, wk.shape[1] // n
        g = qc // HEAD
        half = HEAD // 2
        place = lax.axis_index("sp") * own + jnp.arange(own)
        angle = place.astype(jnp.float32)[:, None] * THETA ** (-jnp.arange(half, dtype=jnp.float32) / half)
        cos, sin = jnp.cos(angle), jnp.sin(angle)
        low = jnp.bfloat16
        anywhere, vmem = pl.BlockSpec(memory_space=pl.ANY), pl.BlockSpec(memory_space=pltpu.VMEM)
        return pl.pallas_call(
            functools.partial(_kernel, n),
            out_shape=jax.ShapeDtypeStruct((own, dim), low),
            in_specs=[anywhere, vmem, vmem, vmem, anywhere, anywhere, anywhere, anywhere],
            out_specs=anywhere,
            scratch_shapes=[
                pltpu.VMEM((own, dim), low),
                pltpu.VMEM((own, dim), low),
                pltpu.VMEM((wk.shape[1] // COLS, dim, COLS), low),
                pltpu.VMEM((WO_SLOTS, qc, dim), low),
                pltpu.VMEM((n, own, HEAD), low),
                pltpu.VMEM((n, HEAD, own), low),
                pltpu.VMEM((n, g * own, HEAD), low),
                pltpu.VMEM((n, own, HEAD), low),
                pltpu.VMEM((n, HEAD + ONES, own), low),
                pltpu.VMEM((n, g * own, HEAD), low),
                pltpu.VMEM((n, own, qc), low),
                pltpu.VMEM((n, own, qc), low),
                pltpu.VMEM((own, dim), jnp.float32),
                pltpu.VMEM((8, g * own), jnp.float32),
                pltpu.VMEM((HEAD + ONES, g * own), jnp.float32),
                *[pltpu.VMEM((2 * own, g * own), jnp.float32)] * 2,
                *[pltpu.VMEM((2 * own, g * own), low)] * 2,
                *[pltpu.VMEM((8, g * own), jnp.float32)] * 4,
                *[pltpu.VMEM((own, HEAD), jnp.float32)] * 2,
                pltpu.SemaphoreType.DMA((1,)),
                pltpu.SemaphoreType.DMA((wk.shape[1] // COLS,)),
                pltpu.SemaphoreType.DMA((WO_SLOTS,)),
                pltpu.SemaphoreType.DMA((4, n)),
                pltpu.SemaphoreType.DMA((4, n)),
            ],
            compiler_params=pltpu.CompilerParams(collective_id=0, has_side_effects=True, vmem_limit_bytes=VMEM),
        )(x, gain.reshape(-1, HEAD), cos, sin, wq, wk, wv, wo)

    tokens, whole = P(("dp", "sp"), None), P(None, None)
    return jax.shard_map(
        step,
        mesh=mesh,
        in_specs=(tokens, P(None), whole, whole, whole, whole),
        out_specs=tokens,
        check_vma=False,
    )
```

```python
import functools

import jax
import jax.numpy as jnp
from jax import lax
from jax.experimental import pallas as pl
from jax.experimental.pallas import tpu as pltpu
from jax.sharding import PartitionSpec as P

HEAD = 128
THETA = 10000
NEG = -1e30
HIDDEN = 2 * NEG
LOG2E = 1.4426950408889634
COLS = 512
ONES = 16
WO_SLOTS = 4
VMEM = 58 * 2**20


def _dot(a, b, ca=1, cb=0):
    return lax.dot_general(a, b, (((ca,), (cb,)), ((), ())), preferred_element_type=jnp.float32)


def _kernel(n, x_hbm, gain_ref, turn_ref, wq, wk, wv, wo, y_hbm,
            xv, av, wbuf, wobuf, ksend, vsend, qsend, kbuf, vbuf, qbuf, osend, obuf, acc, top_s, mix_s, s0, s1, p0, p1, high0, high1, keep0, keep1, cos_s, sin_s,
            xsem, ysem, wsem, wosem, ss, rs):
    me = lax.axis_index("sp")
    s_s, p_s, high_s, keep_s = (s0, s1), (p0, p1), (high0, high1), (keep0, keep1)
    own, dim = xv.shape
    slots = wbuf.shape[0]
    qc, kc = qsend.shape[1] // own * HEAD, HEAD
    q_chunks, k_chunks = wq.shape[1] // COLS, wk.shape[1] // COLS
    q_per, k_per = COLS // qc, COLS // kc
    g = qc // HEAD
    cols = g * own

    side = max(d for d in range(1, n + 1) if n % d == 0 and d * d <= n)
    in_row, down = side // 2, n // side

    def hops(dx, dh, q=None):
        far = [min(2 * dh + i, side - 2 * dh - i) for i in ((0, 1) if q is None else (q,))]
        return min(dx, down - dx) + sum(far) / len(far)

    turns = sorted(((dx, dh) for dh in range(in_row) for dx in range(down)), key=lambda t: (-hops(*t), t[1]))
    kv_turns = sorted(turns, key=lambda t: (min(t[0], down - t[0]), t[1]))
    meetings = sorted(((*t, q) for t in turns for q in range(2)), key=lambda t: hops(*t))

    def partner(c, given, sign=1):
        words = [sum((turn[0] | turn[1] << 3 | (turn[2] if len(turn) > 2 else 0) << 6) << (7 * i) for i, turn in enumerate(given[a:a + 4]))
                 for a in range(0, len(given), 4)]
        word = functools.reduce(lambda low, a: jnp.where(c >= 4 * a, words[a], low), range(1, len(words)), words[0])
        code = lax.shift_right_logical(word, 7 * lax.rem(c, 4))
        row = lax.rem(my_row + down + sign * (code & 7), down)
        return 2 * (row * in_row + lax.rem(my_place + in_row + sign * (lax.shift_right_logical(code, 3) & 7), in_row)), lax.shift_right_logical(code, 6) & 1

    my_row, my_place = lax.div(me, side), lax.div(lax.rem(me, side), 2)

    def meet(s, sign):
        pair, q = partner(s, meetings, sign)
        return pair + lax.rem(me + q, 2)

    asker = lambda s: meet(s, -1)
    answerer = lambda s: meet(s, 1)

    def kv_pairs(c):
        return [partner(2 * c + i, kv_turns)[0] for i in range(2)]

    def kv_chunk(w, c):
        wide = 2 * kc
        return [pltpu.make_async_copy(w.at[:, pl.ds(p * kc, wide)], wbuf.at[c, :, pl.ds(i * wide, wide)], wsem.at[c])
                for i, p in enumerate(kv_pairs(c))]

    def q_chunk(c):
        at, slot = partner(c, turns)[0], lax.rem(c, slots)
        return [pltpu.make_async_copy(wq.at[:, pl.ds(at * qc, COLS)], wbuf.at[slot], wsem.at[slot])]

    def start(given):
        for copy in given:
            copy.start()

    def filled(slot):
        pltpu.make_async_copy(wbuf.at[slot], wbuf.at[slot], wsem.at[slot]).wait()

    get_x = pltpu.make_async_copy(x_hbm, xv, xsem.at[0])
    get_x.start()

    barrier = pltpu.get_barrier_semaphore()

    def greet(s, _):
        pl.semaphore_signal(barrier, inc=1, device_id={"sp": lax.rem(me + s, n)})

    lax.fori_loop(1, n, greet, None)

    start(kv_chunk(wk, 0))
    place = me * own + lax.broadcasted_iota(jnp.int32, (own, HEAD), 0)
    angle = place.astype(jnp.float32) * turn_ref[...]
    cos_s[...] = jnp.cos(angle)
    sin_s[...] = jnp.sin(angle) * jnp.where(lax.broadcasted_iota(jnp.int32, (own, HEAD), 1) < HEAD // 2, -1.0, 1.0)

    get_x.wait()
    for c in range(1, slots):
        start(kv_chunk(wk, c))
    strip = 32
    gain = gain_ref[...].astype(jnp.float32)
    lanes = gain.shape[1]

    def norm(i, _):
        rows = pl.ds(pl.multiple_of(i * strip, strip), strip)
        wide = xv[rows, :].astype(jnp.float32)
        scale = lax.rsqrt(jnp.mean(wide * wide, -1, keepdims=True) + 1e-6)
        for c in range(dim // lanes):
            here = slice(c * lanes, (c + 1) * lanes)
            av[rows, here] = (wide[:, here] * scale * gain[c:c + 1, :]).astype(jnp.bfloat16)

    lax.fori_loop(0, own // strip, norm, None)
    for b in range(n):
        vbuf[b, HEAD:, :] = jnp.ones((ONES, own), jnp.bfloat16)

    def remote(kind, src, dst, to):
        return pltpu.make_async_remote_copy(src_ref=src.at[to], dst_ref=dst.at[me], send_sem=ss.at[kind, to], recv_sem=rs.at[kind, me],
                                            device_id={"sp": to})

    def local(kind, src, dst):
        return pltpu.make_async_copy(src.at[me], dst.at[me], rs.at[kind, me])

    def send(kind, src, dst, to):
        @pl.when(to != me)
        def _():
            remote(kind, src, dst, to).start()

        @pl.when(to == me)
        def _():
            local(kind, src, dst).start()

    def arrived(kind, dst, at):
        pltpu.make_async_copy(dst.at[at], dst.at[at], rs.at[kind, at]).wait()

    def sent(kind, src, s):
        to = lax.rem(me + s, n)
        pltpu.make_async_copy(src.at[to], src.at[to], ss.at[kind, to]).wait()

    vdst = vbuf.at[:, pl.ds(0, HEAD), :]

    def turned(t):
        t = t.astype(jnp.bfloat16).astype(jnp.float32)
        return (t * cos_s[...] + pltpu.roll(t, HEAD // 2, 1) * sin_s[...]).astype(jnp.bfloat16)

    def keys(c, _):
        at = kv_pairs(c)
        filled(c)
        r = _dot(av[...], wbuf[c])
        start(kv_chunk(wv, c))
        for i in range(k_per):
            ksend[at[i // 2] + i % 2] = turned(r[:, i * HEAD:(i + 1) * HEAD])

        @pl.when(c == 0)
        def _():
            pl.semaphore_wait(barrier, n - 1)

        for i in range(k_per):
            send(0, ksend, kbuf, at[i // 2] + i % 2)

    lax.fori_loop(0, k_chunks, keys, None)

    def values(c, _):
        at = kv_pairs(c)
        filled(c)
        r = _dot(av[...], wbuf[c])
        start(q_chunk(c))
        for i in range(k_per):
            vsend[at[i // 2] + i % 2] = r[:, i * HEAD:(i + 1) * HEAD].T.astype(jnp.bfloat16)
        for i in range(k_per):
            send(1, vsend, vdst, at[i // 2] + i % 2)

    lax.fori_loop(0, k_chunks, values, None)

    def queries(c, _):
        at, slot = partner(c, turns)[0], lax.rem(c, slots)
        filled(slot)
        r = _dot(av[...], wbuf[slot])

        @pl.when(c + slots < q_chunks)
        def _():
            start(q_chunk(c + slots))

        for i in range(q_per):
            for h in range(g):
                qsend[at + i, h * own:(h + 1) * own, :] = turned(r[:, (i * g + h) * HEAD:(i * g + h + 1) * HEAD])
    lax.fori_loop(0, q_chunks, queries, None)
    lax.fori_loop(0, n, lambda s, _: send(2, qsend, qbuf, answerer(s)), None)

    def wo_rows(s):
        src = answerer(s)
        slot = lax.rem(s, WO_SLOTS)
        return pltpu.make_async_copy(wo.at[pl.ds(src * qc, qc), :], wobuf.at[slot], wosem.at[slot])

    for s in range(WO_SLOTS):
        wo_rows(s).start()

    acc[...] = xv[...].astype(jnp.float32)
    e = HEAD**-0.5 * LOG2E

    def following(s, b, j):
        last = j == lax.div(b, 2)
        s = jnp.where(last, s + 1, s)
        return s, asker(s), jnp.where(last, 0, j + 1)

    heads = [slice(h * own, (h + 1) * own) for h in range(g)]

    def scores(slot, b, j, masked):
        k = kbuf[pl.ds(2 * j, 2)].reshape(2 * own, HEAD)
        for here in heads:
            sc = _dot(k, qbuf[b, here, :], 1, 1)
            if masked:
                gap = lax.broadcasted_iota(jnp.int32, (2 * own, own), 1) - lax.broadcasted_iota(jnp.int32, (2 * own, own), 0)
                sc = jnp.where(gap >= (2 * j - b) * own, sc, HIDDEN)
            s_s[slot][:, here] = sc
            high_s[slot][0:1, here] = sc.max(axis=0, keepdims=True)

    def weights(slot, j, h):
        here = heads[h]
        old = jnp.where(j == 0, NEG, top_s[0:1, here])
        top = jnp.maximum(old, high_s[slot][0:1, here])
        top_s[0:1, here] = top
        keep_s[slot][0:1, here] = jnp.exp2((old - top) * e)
        p_s[slot][:, here] = jnp.exp2((s_s[slot][:, here] - top) * e).astype(jnp.bfloat16)

    def mix(slot, j, h):
        here = heads[h]
        new = _dot(vbuf[2 * j], p_s[slot][:own, here]) + _dot(vbuf[2 * j + 1], p_s[slot][own:, here])
        mix_s[:, here] = mix_s[:, here] * keep_s[slot][0:1, here] + new

    def finish(b, h):
        here = heads[h]
        out = mix_s[:HEAD, here] * (1 / mix_s[HEAD:HEAD + 1, here])
        osend[b, :, h * HEAD:(h + 1) * HEAD] = out.T.astype(jnp.bfloat16)

    def keys_of(j, _=None):
        for at in (2 * j, 2 * j + 1):
            arrived(0, kbuf, at)
            arrived(1, vdst, at)

    def ready(b, j, seen):
        @pl.when(j == 0)
        def _():
            arrived(2, qbuf, b)

        @pl.when(j > seen)
        def _():
            keys_of(j)

        return jnp.maximum(seen, j)

    def pair(i, at, final=False):
        (s0, b0, j0), (b1, j1), seen = at
        for slot in range(2):
            s2, b2, j2 = following(s0, b0, j0)
            if not final or slot == 0:
                seen = ready(b2, j2, seen)
            for masked in (False, True):
                @pl.when((j2 == lax.div(b2, 2)) == masked)
                def _():
                    if not final or slot == 0:
                        scores(1 - slot, b2, j2, masked)
                    weights(slot, j0, 0)
                    mix(slot, j0, 0)
                    weights(slot, j0, 1)
                    mix(1 - slot, j1, 1)

            @pl.when((j1 == lax.div(b1, 2)) & (i + slot > 0))
            def _():
                finish(b1, 1)
                send(3, osend, obuf, b1)

            @pl.when(j0 == lax.div(b0, 2))
            def _():
                finish(b0, 0)

            (s0, b0, j0), (b1, j1) = (s2, b2, j2), (b0, j0)
        return (s0, b0, j0), (b1, j1), seen

    steps = sum(b // 2 + 1 for b in range(n))
    p_s[1][...] = jnp.zeros(p_s[1].shape, jnp.bfloat16)
    keep_s[1][...] = jnp.zeros(keep_s[1].shape, jnp.float32)
    mix_s[...] = jnp.zeros(mix_s.shape, jnp.float32)
    zero = me - me
    ready(me, zero, zero - 1)
    for masked in (False, True):
        @pl.when((lax.div(me, 2) == 0) == masked)
        def _():
            scores(0, me, 0, masked)
    at = lax.fori_loop(0, steps // 2 - 1, pair, ((zero, me, zero), (me, zero), zero))
    at = pair(1, at, True)
    mix(1, at[1][1], 1)
    finish(at[1][0], 1)
    send(3, osend, obuf, at[1][0])

    half = COLS

    def put(at):
        here = pl.ds(at, half)
        return pltpu.make_async_copy(av.at[:, here], y_hbm.at[:, here], ysem.at[at // half])

    def project(i, final=False):
        pair = []
        for s in (2 * i, 2 * i + 1):
            src = answerer(s)
            arrived(3, obuf, src)
            wo_rows(s).wait()
            pair.append((src, lax.rem(s, WO_SLOTS)))
        for at in range(0, dim, half):
            here = slice(at, at + half)
            new = acc[:, here] + sum(_dot(obuf[src], wobuf[slot, :, here]) for src, slot in pair)
            if final:
                av[:, here] = new.astype(jnp.bfloat16)
                put(at).start()
            else:
                acc[:, here] = new
        if not final:
            for s in (2 * i, 2 * i + 1):
                @pl.when(s + WO_SLOTS < n)
                def _():
                    wo_rows(s + WO_SLOTS).start()

    lax.fori_loop(0, n // 2 - 1, lambda i, _: project(i), None)
    project(n // 2 - 1 + zero, True)

    def drain(s, _):
        sent(0, ksend, s)
        sent(1, vsend, s)
        sent(2, qsend, s)
        sent(3, osend, s)

    lax.fori_loop(1, n, drain, None)
    for at in range(0, dim, half):
        put(at).wait()


def solution(mesh):
    n = mesh.shape["sp"]

    def step(x, gain, wq, wk, wv, wo):
        own, dim = x.shape
        qc, kc = wq.shape[1] // n, wk.shape[1] // n
        g = qc // HEAD
        half = HEAD // 2
        turn = THETA ** (-(jnp.arange(HEAD) % half).astype(jnp.float32) / half)
        low = jnp.bfloat16
        anywhere, vmem = pl.BlockSpec(memory_space=pl.ANY), pl.BlockSpec(memory_space=pltpu.VMEM)
        return pl.pallas_call(
            functools.partial(_kernel, n),
            out_shape=jax.ShapeDtypeStruct((own, dim), low),
            in_specs=[anywhere, vmem, vmem, anywhere, anywhere, anywhere, anywhere],
            out_specs=anywhere,
            scratch_shapes=[
                pltpu.VMEM((own, dim), low),
                pltpu.VMEM((own, dim), low),
                pltpu.VMEM((wk.shape[1] // COLS, dim, COLS), low),
                pltpu.VMEM((WO_SLOTS, qc, dim), low),
                pltpu.VMEM((n, own, HEAD), low),
                pltpu.VMEM((n, HEAD, own), low),
                pltpu.VMEM((n, g * own, HEAD), low),
                pltpu.VMEM((n, own, HEAD), low),
                pltpu.VMEM((n, HEAD + ONES, own), low),
                pltpu.VMEM((n, g * own, HEAD), low),
                pltpu.VMEM((n, own, qc), low),
                pltpu.VMEM((n, own, qc), low),
                pltpu.VMEM((own, dim), jnp.float32),
                pltpu.VMEM((8, g * own), jnp.float32),
                pltpu.VMEM((HEAD + ONES, g * own), jnp.float32),
                *[pltpu.VMEM((2 * own, g * own), jnp.float32)] * 2,
                *[pltpu.VMEM((2 * own, g * own), low)] * 2,
                *[pltpu.VMEM((8, g * own), jnp.float32)] * 4,
                *[pltpu.VMEM((own, HEAD), jnp.float32)] * 2,
                pltpu.SemaphoreType.DMA((1,)),
                pltpu.SemaphoreType.DMA((dim // COLS,)),
                pltpu.SemaphoreType.DMA((wk.shape[1] // COLS,)),
                pltpu.SemaphoreType.DMA((WO_SLOTS,)),
                pltpu.SemaphoreType.DMA((4, n)),
                pltpu.SemaphoreType.DMA((4, n)),
            ],
            compiler_params=pltpu.CompilerParams(collective_id=0, has_side_effects=True, vmem_limit_bytes=VMEM),
        )(x, gain.reshape(-1, HEAD), turn.reshape(1, HEAD), wq, wk, wv, wo)

    tokens, whole = P(("dp", "sp"), None), P(None, None)
    return jax.shard_map(
        step,
        mesh=mesh,
        in_specs=(tokens, P(None), whole, whole, whole, whole),
        out_specs=tokens,
        check_vma=False,
    )
```

```python
import functools

import jax
import jax.numpy as jnp
from jax import lax
from jax.experimental import pallas as pl
from jax.experimental.pallas import tpu as pltpu
from jax.sharding import PartitionSpec as P

HEAD = 128
THETA = 10000
NEG = -1e30
HIDDEN = 2 * NEG
LOG2E = 1.4426950408889634
COLS = 512
ONES = 16
WO_SLOTS = 6
VMEM = 67043328


def _dot(a, b, ca=1, cb=0):
    return lax.dot_general(a, b, (((ca,), (cb,)), ((), ())), preferred_element_type=jnp.float32)


def _kernel(n, x_hbm, gain_ref, turn_ref, wq, wk, wv, wo, y_hbm,
            xv, av, wbuf, wobuf, ksend, vsend, qsend, kbuf, vbuf, qbuf, osend, obuf, acc, top_s, mix_s, s0, s1, p0, p1, high0, high1, keep0, keep1, cos_s, sin_s,
            xsem, ysem, wsem, wosem, ss, rs):
    me = lax.axis_index("sp")
    s_s, p_s, high_s, keep_s = (s0, s1), (p0, p1), (high0, high1), (keep0, keep1)
    own, dim = xv.shape
    slots = wbuf.shape[0]
    qc, kc = qsend.shape[1] // own * HEAD, HEAD
    q_chunks, k_chunks = wq.shape[1] // COLS, wk.shape[1] // COLS
    q_per, k_per = COLS // qc, COLS // kc
    g = qc // HEAD
    cols = g * own

    side = max(d for d in range(1, n + 1) if n % d == 0 and d * d <= n)
    in_row, down = side // 2, n // side

    def hops(dx, dh, q=None):
        far = [min(2 * dh + i, side - 2 * dh - i) for i in ((0, 1) if q is None else (q,))]
        return min(dx, down - dx) + sum(far) / len(far)

    turns = sorted(((dx, dh) for dh in range(in_row) for dx in range(down)), key=lambda t: (hops(*t), t[1]))
    kv_turns = sorted(turns, key=lambda t: (min(t[0], down - t[0]), t[1]))
    meetings = sorted(((*t, q) for t in turns for q in range(2)), key=lambda t: hops(*t))

    def partner(c, given, sign=1):
        words = [sum((turn[0] | turn[1] << 3 | (turn[2] if len(turn) > 2 else 0) << 6) << (7 * i) for i, turn in enumerate(given[a:a + 4]))
                 for a in range(0, len(given), 4)]
        word = functools.reduce(lambda low, a: jnp.where(c >= 4 * a, words[a], low), range(1, len(words)), words[0])
        code = lax.shift_right_logical(word, 7 * lax.rem(c, 4))
        row = lax.rem(my_row + down + sign * (code & 7), down)
        return 2 * (row * in_row + lax.rem(my_place + in_row + sign * (lax.shift_right_logical(code, 3) & 7), in_row)), lax.shift_right_logical(code, 6) & 1

    my_row, my_place = lax.div(me, side), lax.div(lax.rem(me, side), 2)

    def meet(s, sign):
        pair, q = partner(s, meetings, sign)
        return pair + lax.rem(me + q, 2)

    asker = lambda s: meet(s, -1)
    answerer = lambda s: meet(s, 1)

    def kv_pairs(c):
        return [partner(2 * c + i, kv_turns)[0] for i in range(2)]

    def kv_chunk(w, c):
        wide = 2 * kc
        return [pltpu.make_async_copy(w.at[:, pl.ds(p * kc, wide)], wbuf.at[c, :, pl.ds(i * wide, wide)], wsem.at[c])
                for i, p in enumerate(kv_pairs(c))]

    def q_chunk(c):
        at, slot = partner(c, turns)[0], lax.rem(c, slots)
        return [pltpu.make_async_copy(wq.at[:, pl.ds(at * qc, COLS)], wbuf.at[slot], wsem.at[slot])]

    def start(given):
        for copy in given:
            copy.start()

    def filled(slot):
        pltpu.make_async_copy(wbuf.at[slot], wbuf.at[slot], wsem.at[slot]).wait()

    get_x = pltpu.make_async_copy(x_hbm, xv, xsem.at[0])
    get_x.start()

    barrier = pltpu.get_barrier_semaphore()

    def greet(s, _):
        pl.semaphore_signal(barrier, inc=1, device_id={"sp": lax.rem(me + s, n)})

    lax.fori_loop(1, n, greet, None)

    start(kv_chunk(wk, 0))
    place = me * own + lax.broadcasted_iota(jnp.int32, (own, HEAD), 0)
    angle = place.astype(jnp.float32) * turn_ref[...]
    cos_s[...] = jnp.cos(angle)
    sin_s[...] = jnp.sin(angle) * jnp.where(lax.broadcasted_iota(jnp.int32, (own, HEAD), 1) < HEAD // 2, -1.0, 1.0)

    get_x.wait()
    for c in range(1, slots):
        start(kv_chunk(wk, c))
    strip = 32
    gain = gain_ref[...].astype(jnp.float32)
    lanes = gain.shape[1]

    def norm(i, _):
        rows = pl.ds(pl.multiple_of(i * strip, strip), strip)
        wide = xv[rows, :].astype(jnp.float32)
        scale = lax.rsqrt(jnp.mean(wide * wide, -1, keepdims=True) + 1e-6)
        for c in range(dim // lanes):
            here = slice(c * lanes, (c + 1) * lanes)
            av[rows, here] = (wide[:, here] * scale * gain[c:c + 1, :]).astype(jnp.bfloat16)

    lax.fori_loop(0, own // strip, norm, None)
    for b in range(n):
        vbuf[b, HEAD:, :] = jnp.ones((ONES, own), jnp.bfloat16)

    def remote(kind, src, dst, to):
        return pltpu.make_async_remote_copy(src_ref=src.at[to], dst_ref=dst.at[me], send_sem=ss.at[kind, to], recv_sem=rs.at[kind, me],
                                            device_id={"sp": to})

    def local(kind, src, dst):
        return pltpu.make_async_copy(src.at[me], dst.at[me], rs.at[kind, me])

    def send(kind, src, dst, to):
        @pl.when(to != me)
        def _():
            remote(kind, src, dst, to).start()

        @pl.when(to == me)
        def _():
            local(kind, src, dst).start()

    def arrived(kind, dst, at):
        pltpu.make_async_copy(dst.at[at], dst.at[at], rs.at[kind, at]).wait()

    def sent(kind, src, s):
        to = lax.rem(me + s, n)
        pltpu.make_async_copy(src.at[to], src.at[to], ss.at[kind, to]).wait()

    vdst = vbuf.at[:, pl.ds(0, HEAD), :]

    def turned(t):
        t = t.astype(jnp.bfloat16).astype(jnp.float32)
        return (t * cos_s[...] + pltpu.roll(t, HEAD // 2, 1) * sin_s[...]).astype(jnp.bfloat16)

    def keys(c, _):
        at = kv_pairs(c)
        filled(c)
        r = _dot(av[...], wbuf[c])
        start(kv_chunk(wv, c))
        for i in range(k_per):
            ksend[at[i // 2] + i % 2] = turned(r[:, i * HEAD:(i + 1) * HEAD])

        @pl.when(c == 0)
        def _():
            pl.semaphore_wait(barrier, n - 1)

        for i in range(k_per):
            send(0, ksend, kbuf, at[i // 2] + i % 2)

    lax.fori_loop(0, k_chunks, keys, None)

    def values(c, _):
        at = kv_pairs(c)
        filled(c)
        r = _dot(av[...], wbuf[c])
        start(q_chunk(c))
        for i in range(k_per):
            vsend[at[i // 2] + i % 2] = r[:, i * HEAD:(i + 1) * HEAD].T.astype(jnp.bfloat16)
        for i in range(k_per):
            send(1, vsend, vdst, at[i // 2] + i % 2)

    lax.fori_loop(0, k_chunks, values, None)

    def queries(c, _):
        at, slot = partner(c, turns)[0], lax.rem(c, slots)
        filled(slot)
        r = _dot(av[...], wbuf[slot])

        @pl.when(c + slots < q_chunks)
        def _():
            start(q_chunk(c + slots))

        for i in range(q_per):
            for h in range(g):
                qsend[at + i, h * own:(h + 1) * own, :] = turned(r[:, (i * g + h) * HEAD:(i * g + h + 1) * HEAD])
        for i in range(q_per):
            send(2, qsend, qbuf, at + i)
    lax.fori_loop(0, q_chunks, queries, None)

    def wo_rows(s):
        src = answerer(s)
        slot = lax.rem(s, WO_SLOTS)
        return pltpu.make_async_copy(wo.at[pl.ds(src * qc, qc), :], wobuf.at[slot], wosem.at[slot])

    for s in range(WO_SLOTS):
        wo_rows(s).start()

    acc[...] = xv[...].astype(jnp.float32)
    e = HEAD**-0.5 * LOG2E

    def following(s, b, j):
        last = j == lax.div(b, 2)
        s = jnp.where(last, s + 1, s)
        return s, asker(s), jnp.where(last, 0, j + 1)

    heads = [slice(h * own, (h + 1) * own) for h in range(g)]

    def scores(slot, b, j, masked):
        k = kbuf[pl.ds(2 * j, 2)].reshape(2 * own, HEAD)
        for here in heads:
            sc = _dot(k, qbuf[b, here, :], 1, 1)
            if masked:
                gap = lax.broadcasted_iota(jnp.int32, (2 * own, own), 1) - lax.broadcasted_iota(jnp.int32, (2 * own, own), 0)
                sc = jnp.where(gap >= (2 * j - b) * own, sc, HIDDEN)
            s_s[slot][:, here] = sc
            high_s[slot][0:1, here] = sc.max(axis=0, keepdims=True)

    def weights(slot, j, h):
        here = heads[h]
        old = jnp.where(j == 0, NEG, top_s[0:1, here])
        top = jnp.maximum(old, high_s[slot][0:1, here])
        top_s[0:1, here] = top
        keep_s[slot][0:1, here] = jnp.exp2((old - top) * e)
        p_s[slot][:, here] = jnp.exp2((s_s[slot][:, here] - top) * e).astype(jnp.bfloat16)

    def mix(slot, j, h):
        here = heads[h]
        new = _dot(vbuf[2 * j], p_s[slot][:own, here]) + _dot(vbuf[2 * j + 1], p_s[slot][own:, here])
        mix_s[:, here] = mix_s[:, here] * keep_s[slot][0:1, here] + new

    def finish(b, h):
        here = heads[h]
        out = mix_s[:HEAD, here] * (1 / mix_s[HEAD:HEAD + 1, here])
        osend[b, :, h * HEAD:(h + 1) * HEAD] = out.T.astype(jnp.bfloat16)

    def keys_of(j, _=None):
        for at in (2 * j, 2 * j + 1):
            arrived(0, kbuf, at)
            arrived(1, vdst, at)

    def ready(b, j, seen):
        @pl.when(j == 0)
        def _():
            arrived(2, qbuf, b)

        @pl.when(j > seen)
        def _():
            keys_of(j)

        return jnp.maximum(seen, j)

    def pair(i, at, final=False):
        (s0, b0, j0), (b1, j1), seen = at
        for slot in range(2):
            s2, b2, j2 = following(s0, b0, j0)
            if not final or slot == 0:
                seen = ready(b2, j2, seen)
            for masked in (False, True):
                @pl.when((j2 == lax.div(b2, 2)) == masked)
                def _():
                    if not final or slot == 0:
                        scores(1 - slot, b2, j2, masked)
                    weights(slot, j0, 0)
                    mix(slot, j0, 0)
                    weights(slot, j0, 1)
                    mix(1 - slot, j1, 1)

            @pl.when((j1 == lax.div(b1, 2)) & (i + slot > 0))
            def _():
                finish(b1, 1)
                send(3, osend, obuf, b1)

            @pl.when(j0 == lax.div(b0, 2))
            def _():
                finish(b0, 0)

            (s0, b0, j0), (b1, j1) = (s2, b2, j2), (b0, j0)
        return (s0, b0, j0), (b1, j1), seen

    steps = sum(b // 2 + 1 for b in range(n))
    p_s[1][...] = jnp.zeros(p_s[1].shape, jnp.bfloat16)
    keep_s[1][...] = jnp.zeros(keep_s[1].shape, jnp.float32)
    mix_s[...] = jnp.zeros(mix_s.shape, jnp.float32)
    zero = me - me
    ready(me, zero, zero - 1)
    for masked in (False, True):
        @pl.when((lax.div(me, 2) == 0) == masked)
        def _():
            scores(0, me, 0, masked)
    at = lax.fori_loop(0, steps // 2 - 1, pair, ((zero, me, zero), (me, zero), zero))
    at = pair(1, at, True)
    mix(1, at[1][1], 1)
    finish(at[1][0], 1)
    send(3, osend, obuf, at[1][0])

    half = COLS

    def put(at):
        here = pl.ds(at, half)
        return pltpu.make_async_copy(av.at[:, here], y_hbm.at[:, here], ysem.at[at // half])

    def project(i, final=False):
        pair = []
        for s in (2 * i, 2 * i + 1):
            src = answerer(s)
            arrived(3, obuf, src)
            wo_rows(s).wait()
            pair.append((src, lax.rem(s, WO_SLOTS)))
        for at in range(0, dim, half):
            here = slice(at, at + half)
            new = acc[:, here] + sum(_dot(obuf[src], wobuf[slot, :, here]) for src, slot in pair)
            if final:
                av[:, here] = new.astype(jnp.bfloat16)
                put(at).start()
            else:
                acc[:, here] = new
        if not final:
            for s in (2 * i, 2 * i + 1):
                @pl.when(s + WO_SLOTS < n)
                def _():
                    wo_rows(s + WO_SLOTS).start()

    lax.fori_loop(0, n // 2 - 1, lambda i, _: project(i), None)
    project(n // 2 - 1 + zero, True)

    def drain(s, _):
        sent(0, ksend, s)
        sent(1, vsend, s)
        sent(2, qsend, s)
        sent(3, osend, s)

    lax.fori_loop(1, n, drain, None)
    for at in range(0, dim, half):
        put(at).wait()


def _copy(parts, y_ref, out_ref, held, came, went):
    rows = held.shape[0] // parts
    come = lambda i: pltpu.make_async_copy(y_ref.at[pl.ds(i * rows, rows)], held.at[pl.ds(i * rows, rows)], came.at[i])
    go = lambda i: pltpu.make_async_copy(held.at[pl.ds(i * rows, rows)], out_ref.at[pl.ds(i * rows, rows)], went.at[i])
    for i in range(parts):
        come(i).start()
    for i in range(parts):
        come(i).wait()
        go(i).start()
    for i in range(parts):
        go(i).wait()


def solution(mesh):
    n = mesh.shape["sp"]

    def step(x, gain, wq, wk, wv, wo):
        own, dim = x.shape
        qc, kc = wq.shape[1] // n, wk.shape[1] // n
        g = qc // HEAD
        half = HEAD // 2
        turn = THETA ** (-(jnp.arange(HEAD) % half).astype(jnp.float32) / half)
        low = jnp.bfloat16
        anywhere, vmem = pl.BlockSpec(memory_space=pl.ANY), pl.BlockSpec(memory_space=pltpu.VMEM)
        y = pl.pallas_call(
            functools.partial(_kernel, n),
            out_shape=jax.ShapeDtypeStruct((own, dim), low),
            in_specs=[anywhere, vmem, vmem, anywhere, anywhere, anywhere, anywhere],
            out_specs=anywhere,
            scratch_shapes=[
                pltpu.VMEM((own, dim), low),
                pltpu.VMEM((own, dim), low),
                pltpu.VMEM((wk.shape[1] // COLS, dim, COLS), low),
                pltpu.VMEM((WO_SLOTS, qc, dim), low),
                pltpu.VMEM((n, own, HEAD), low),
                pltpu.VMEM((n, HEAD, own), low),
                pltpu.VMEM((n, g * own, HEAD), low),
                pltpu.VMEM((n, own, HEAD), low),
                pltpu.VMEM((n, HEAD + ONES, own), low),
                pltpu.VMEM((n, g * own, HEAD), low),
                pltpu.VMEM((n, own, qc), low),
                pltpu.VMEM((n, own, qc), low),
                pltpu.VMEM((own, dim), jnp.float32),
                pltpu.VMEM((8, g * own), jnp.float32),
                pltpu.VMEM((HEAD + ONES, g * own), jnp.float32),
                *[pltpu.VMEM((2 * own, g * own), jnp.float32)] * 2,
                *[pltpu.VMEM((2 * own, g * own), low)] * 2,
                *[pltpu.VMEM((8, g * own), jnp.float32)] * 4,
                *[pltpu.VMEM((own, HEAD), jnp.float32)] * 2,
                pltpu.SemaphoreType.DMA((1,)),
                pltpu.SemaphoreType.DMA((dim // COLS,)),
                pltpu.SemaphoreType.DMA((wk.shape[1] // COLS,)),
                pltpu.SemaphoreType.DMA((WO_SLOTS,)),
                pltpu.SemaphoreType.DMA((4, n)),
                pltpu.SemaphoreType.DMA((4, n)),
            ],
            compiler_params=pltpu.CompilerParams(collective_id=0, has_side_effects=True, vmem_limit_bytes=VMEM),
        )(x, gain.reshape(-1, HEAD), turn.reshape(1, HEAD), wq, wk, wv, wo)
        parts = 4
        return pl.pallas_call(
            functools.partial(_copy, parts),
            out_shape=jax.ShapeDtypeStruct((own, dim), low),
            in_specs=[anywhere],
            out_specs=anywhere,
            scratch_shapes=[pltpu.VMEM((own, dim), low), pltpu.SemaphoreType.DMA((parts,)), pltpu.SemaphoreType.DMA((parts,))],
            compiler_params=pltpu.CompilerParams(vmem_limit_bytes=VMEM),
        )(y)

    tokens, whole = P(("dp", "sp"), None), P(None, None)
    return jax.shard_map(
        step,
        mesh=mesh,
        in_specs=(tokens, P(None), whole, whole, whole, whole),
        out_specs=tokens,
        check_vma=False,
    )
```

```python
import functools

import jax
import jax.numpy as jnp
from jax import lax
from jax.experimental import pallas as pl
from jax.experimental.pallas import tpu as pltpu
from jax.sharding import PartitionSpec as P

HEAD = 128
THETA = 10000
NEG = -1e30
HIDDEN = 2 * NEG
LOG2E = 1.4426950408889634
COLS = 512
ONES = 16
WO_SLOTS = 6
VMEM = 67043328


def _dot(a, b, ca=1, cb=0):
    return lax.dot_general(a, b, (((ca,), (cb,)), ((), ())), preferred_element_type=jnp.float32)


def _kernel(n, x_hbm, gain_ref, turn_ref, wq, wk, wv, wo, y_hbm,
            xv, av, wbuf, wobuf, ksend, vsend, qsend, kbuf, vbuf, qbuf, osend, obuf, acc, top_s, mix_s, s0, s1, p0, p1, high0, high1, keep0, keep1, cos_s, sin_s,
            xsem, ysem, wsem, wosem, ss, rs):
    me = lax.axis_index("sp")
    s_s, p_s, high_s, keep_s = (s0, s1), (p0, p1), (high0, high1), (keep0, keep1)
    own, dim = xv.shape
    slots = wbuf.shape[0]
    qc, kc = qsend.shape[1] // own * HEAD, HEAD
    q_chunks, k_chunks = wq.shape[1] // COLS, wk.shape[1] // COLS
    q_per, k_per = COLS // qc, COLS // kc
    g = qc // HEAD
    cols = g * own

    side = max(d for d in range(1, n + 1) if n % d == 0 and d * d <= n)
    in_row, down = side // 2, n // side

    def hops(dx, dh, q=None):
        far = [min(2 * dh + i, side - 2 * dh - i) for i in ((0, 1) if q is None else (q,))]
        return min(dx, down - dx) + sum(far) / len(far)

    turns = sorted(((dx, dh) for dh in range(in_row) for dx in range(down)), key=lambda t: (hops(*t), t[1]))
    q_turns = [(*t, min(range(2), key=lambda q: hops(*t, q))) for t in turns]
    kv_turns = sorted(turns, key=lambda t: (min(t[0], down - t[0]), t[1]))
    meetings = sorted(((*t, q) for t in turns for q in range(2)), key=lambda t: hops(*t))

    def partner(c, given, sign=1):
        words = [sum((turn[0] | turn[1] << 3 | (turn[2] if len(turn) > 2 else 0) << 6) << (7 * i) for i, turn in enumerate(given[a:a + 4]))
                 for a in range(0, len(given), 4)]
        word = functools.reduce(lambda low, a: jnp.where(c >= 4 * a, words[a], low), range(1, len(words)), words[0])
        code = lax.shift_right_logical(word, 7 * lax.rem(c, 4))
        row = lax.rem(my_row + down + sign * (code & 7), down)
        return 2 * (row * in_row + lax.rem(my_place + in_row + sign * (lax.shift_right_logical(code, 3) & 7), in_row)), lax.shift_right_logical(code, 6) & 1

    my_row, my_place = lax.div(me, side), lax.div(lax.rem(me, side), 2)

    def meet(s, sign):
        pair, q = partner(s, meetings, sign)
        return pair + lax.rem(me + q, 2)

    asker = lambda s: meet(s, -1)
    answerer = lambda s: meet(s, 1)

    def kv_pairs(c):
        return [partner(2 * c + i, kv_turns)[0] for i in range(2)]

    def kv_chunk(w, c):
        wide = 2 * kc
        return [pltpu.make_async_copy(w.at[:, pl.ds(p * kc, wide)], wbuf.at[c, :, pl.ds(i * wide, wide)], wsem.at[c])
                for i, p in enumerate(kv_pairs(c))]

    def q_chunk(c):
        at, slot = partner(c, turns)[0], lax.rem(c, slots)
        return [pltpu.make_async_copy(wq.at[:, pl.ds(at * qc, COLS)], wbuf.at[slot], wsem.at[slot])]

    def start(given):
        for copy in given:
            copy.start()

    def filled(slot):
        pltpu.make_async_copy(wbuf.at[slot], wbuf.at[slot], wsem.at[slot]).wait()

    get_x = pltpu.make_async_copy(x_hbm, xv, xsem.at[0])
    get_x.start()

    barrier = pltpu.get_barrier_semaphore()

    def greet(s, _):
        pl.semaphore_signal(barrier, inc=1, device_id={"sp": lax.rem(me + s, n)})

    lax.fori_loop(1, n, greet, None)

    start(kv_chunk(wk, 0))
    place = me * own + lax.broadcasted_iota(jnp.int32, (own, HEAD), 0)
    angle = place.astype(jnp.float32) * turn_ref[...]
    cos_s[...] = jnp.cos(angle)
    sin_s[...] = jnp.sin(angle) * jnp.where(lax.broadcasted_iota(jnp.int32, (own, HEAD), 1) < HEAD // 2, -1.0, 1.0)

    get_x.wait()
    for c in range(1, slots):
        start(kv_chunk(wk, c))
    strip = 32
    gain = gain_ref[...].astype(jnp.float32)
    lanes = gain.shape[1]

    def norm(i, _):
        rows = pl.ds(pl.multiple_of(i * strip, strip), strip)
        wide = xv[rows, :].astype(jnp.float32)
        scale = lax.rsqrt(jnp.mean(wide * wide, -1, keepdims=True) + 1e-6)
        for c in range(dim // lanes):
            here = slice(c * lanes, (c + 1) * lanes)
            av[rows, here] = (wide[:, here] * scale * gain[c:c + 1, :]).astype(jnp.bfloat16)

    lax.fori_loop(0, own // strip, norm, None)
    for b in range(n):
        vbuf[b, HEAD:, :] = jnp.ones((ONES, own), jnp.bfloat16)

    def remote(kind, src, dst, to):
        return pltpu.make_async_remote_copy(src_ref=src.at[to], dst_ref=dst.at[me], send_sem=ss.at[kind, to], recv_sem=rs.at[kind, me],
                                            device_id={"sp": to})

    def local(kind, src, dst):
        return pltpu.make_async_copy(src.at[me], dst.at[me], rs.at[kind, me])

    def send(kind, src, dst, to):
        @pl.when(to != me)
        def _():
            remote(kind, src, dst, to).start()

        @pl.when(to == me)
        def _():
            local(kind, src, dst).start()

    def arrived(kind, dst, at):
        pltpu.make_async_copy(dst.at[at], dst.at[at], rs.at[kind, at]).wait()

    def sent(kind, src, s):
        to = lax.rem(me + s, n)
        pltpu.make_async_copy(src.at[to], src.at[to], ss.at[kind, to]).wait()

    vdst = vbuf.at[:, pl.ds(0, HEAD), :]

    def turned(t):
        t = t.astype(jnp.bfloat16).astype(jnp.float32)
        return (t * cos_s[...] + pltpu.roll(t, HEAD // 2, 1) * sin_s[...]).astype(jnp.bfloat16)

    def keys(c, _):
        at = kv_pairs(c)
        filled(c)
        r = _dot(av[...], wbuf[c])
        start(kv_chunk(wv, c))
        for i in range(k_per):
            ksend[at[i // 2] + i % 2] = turned(r[:, i * HEAD:(i + 1) * HEAD])

        @pl.when(c == 0)
        def _():
            pl.semaphore_wait(barrier, n - 1)

        for i in range(k_per):
            send(0, ksend, kbuf, at[i // 2] + i % 2)

    lax.fori_loop(0, k_chunks, keys, None)

    def values(c, _):
        at = kv_pairs(c)
        filled(c)
        r = _dot(av[...], wbuf[c])
        start(q_chunk(c))
        for i in range(k_per):
            vsend[at[i // 2] + i % 2] = r[:, i * HEAD:(i + 1) * HEAD].T.astype(jnp.bfloat16)
        for i in range(k_per):
            send(1, vsend, vdst, at[i // 2] + i % 2)

    lax.fori_loop(0, k_chunks, values, None)

    def queries(c, _):
        (at, near), slot = partner(c, q_turns), lax.rem(c, slots)
        filled(slot)
        r = _dot(av[...], wbuf[slot])

        @pl.when(c + slots < q_chunks)
        def _():
            start(q_chunk(c + slots))

        for i in range(q_per):
            for h in range(g):
                qsend[at + i, h * own:(h + 1) * own, :] = turned(r[:, (i * g + h) * HEAD:(i * g + h + 1) * HEAD])
        for i in range(q_per):
            send(2, qsend, qbuf, at + lax.rem(me + near + i, 2))
    lax.fori_loop(0, q_chunks, queries, None)

    def wo_rows(s):
        src = answerer(s)
        slot = lax.rem(s, WO_SLOTS)
        return pltpu.make_async_copy(wo.at[pl.ds(src * qc, qc), :], wobuf.at[slot], wosem.at[slot])

    for s in range(WO_SLOTS):
        wo_rows(s).start()

    acc[...] = xv[...].astype(jnp.float32)
    e = HEAD**-0.5 * LOG2E

    def following(s, b, j):
        last = j == lax.div(b, 2)
        s = jnp.where(last, s + 1, s)
        return s, asker(s), jnp.where(last, 0, j + 1)

    heads = [slice(h * own, (h + 1) * own) for h in range(g)]

    def scores(slot, b, j, masked):
        k = kbuf[pl.ds(2 * j, 2)].reshape(2 * own, HEAD)
        for here in heads:
            sc = _dot(k, qbuf[b, here, :], 1, 1)
            if masked:
                gap = lax.broadcasted_iota(jnp.int32, (2 * own, own), 1) - lax.broadcasted_iota(jnp.int32, (2 * own, own), 0)
                sc = jnp.where(gap >= (2 * j - b) * own, sc, HIDDEN)
            s_s[slot][:, here] = sc
            high_s[slot][0:1, here] = sc.max(axis=0, keepdims=True)

    def weights(slot, j, h):
        here = heads[h]
        old = jnp.where(j == 0, NEG, top_s[0:1, here])
        top = jnp.maximum(old, high_s[slot][0:1, here])
        top_s[0:1, here] = top
        keep_s[slot][0:1, here] = jnp.exp2((old - top) * e)
        p_s[slot][:, here] = jnp.exp2((s_s[slot][:, here] - top) * e).astype(jnp.bfloat16)

    def mix(slot, j, h):
        here = heads[h]
        new = _dot(vbuf[2 * j], p_s[slot][:own, here]) + _dot(vbuf[2 * j + 1], p_s[slot][own:, here])
        mix_s[:, here] = mix_s[:, here] * keep_s[slot][0:1, here] + new

    def finish(b, h):
        here = heads[h]
        out = mix_s[:HEAD, here] * (1 / mix_s[HEAD:HEAD + 1, here])
        osend[b, :, h * HEAD:(h + 1) * HEAD] = out.T.astype(jnp.bfloat16)

    def keys_of(j, _=None):
        for at in (2 * j, 2 * j + 1):
            arrived(0, kbuf, at)
            arrived(1, vdst, at)

    def ready(b, j, seen):
        @pl.when(j == 0)
        def _():
            arrived(2, qbuf, b)

        @pl.when(j > seen)
        def _():
            keys_of(j)

        return jnp.maximum(seen, j)

    def pair(i, at, final=False):
        (s0, b0, j0), (b1, j1), seen = at
        for slot in range(2):
            s2, b2, j2 = following(s0, b0, j0)
            if not final or slot == 0:
                seen = ready(b2, j2, seen)
            for masked in (False, True):
                @pl.when((j2 == lax.div(b2, 2)) == masked)
                def _():
                    if not final or slot == 0:
                        scores(1 - slot, b2, j2, masked)
                    weights(slot, j0, 0)
                    mix(slot, j0, 0)
                    weights(slot, j0, 1)
                    mix(1 - slot, j1, 1)

            @pl.when((j1 == lax.div(b1, 2)) & (i + slot > 0))
            def _():
                finish(b1, 1)
                send(3, osend, obuf, b1)

            @pl.when(j0 == lax.div(b0, 2))
            def _():
                finish(b0, 0)

            (s0, b0, j0), (b1, j1) = (s2, b2, j2), (b0, j0)
        return (s0, b0, j0), (b1, j1), seen

    steps = sum(b // 2 + 1 for b in range(n))
    p_s[1][...] = jnp.zeros(p_s[1].shape, jnp.bfloat16)
    keep_s[1][...] = jnp.zeros(keep_s[1].shape, jnp.float32)
    mix_s[...] = jnp.zeros(mix_s.shape, jnp.float32)
    zero = me - me
    ready(me, zero, zero - 1)
    for masked in (False, True):
        @pl.when((lax.div(me, 2) == 0) == masked)
        def _():
            scores(0, me, 0, masked)
    at = lax.fori_loop(0, steps // 2 - 1, pair, ((zero, me, zero), (me, zero), zero))
    at = pair(1, at, True)
    mix(1, at[1][1], 1)
    finish(at[1][0], 1)
    send(3, osend, obuf, at[1][0])

    half = COLS

    def put(at):
        here = pl.ds(at, half)
        return pltpu.make_async_copy(av.at[:, here], y_hbm.at[:, here], ysem.at[at // half])

    def project(i, final=False):
        pair = []
        for s in (2 * i, 2 * i + 1):
            src = answerer(s)
            arrived(3, obuf, src)
            wo_rows(s).wait()
            pair.append((src, lax.rem(s, WO_SLOTS)))
        for at in range(0, dim, half):
            here = slice(at, at + half)
            new = acc[:, here] + sum(_dot(obuf[src], wobuf[slot, :, here]) for src, slot in pair)
            if final:
                av[:, here] = new.astype(jnp.bfloat16)
                put(at).start()
            else:
                acc[:, here] = new
        if not final:
            for s in (2 * i, 2 * i + 1):
                @pl.when(s + WO_SLOTS < n)
                def _():
                    wo_rows(s + WO_SLOTS).start()

    lax.fori_loop(0, n // 2 - 1, lambda i, _: project(i), None)
    project(n // 2 - 1 + zero, True)

    def drain(s, _):
        sent(0, ksend, s)
        sent(1, vsend, s)
        sent(2, qsend, s)
        sent(3, osend, s)

    lax.fori_loop(1, n, drain, None)
    for at in range(0, dim, half):
        put(at).wait()


def _copy(parts, y_ref, out_ref, held, came, went):
    rows = held.shape[0] // parts
    come = lambda i: pltpu.make_async_copy(y_ref.at[pl.ds(i * rows, rows)], held.at[pl.ds(i * rows, rows)], came.at[i])
    go = lambda i: pltpu.make_async_copy(held.at[pl.ds(i * rows, rows)], out_ref.at[pl.ds(i * rows, rows)], went.at[i])
    for i in range(parts):
        come(i).start()
    for i in range(parts):
        come(i).wait()
        go(i).start()
    for i in range(parts):
        go(i).wait()


def solution(mesh):
    n = mesh.shape["sp"]

    def step(x, gain, wq, wk, wv, wo):
        own, dim = x.shape
        qc, kc = wq.shape[1] // n, wk.shape[1] // n
        g = qc // HEAD
        half = HEAD // 2
        turn = THETA ** (-(jnp.arange(HEAD) % half).astype(jnp.float32) / half)
        low = jnp.bfloat16
        anywhere, vmem = pl.BlockSpec(memory_space=pl.ANY), pl.BlockSpec(memory_space=pltpu.VMEM)
        y = pl.pallas_call(
            functools.partial(_kernel, n),
            out_shape=jax.ShapeDtypeStruct((own, dim), low),
            in_specs=[anywhere, vmem, vmem, anywhere, anywhere, anywhere, anywhere],
            out_specs=anywhere,
            scratch_shapes=[
                pltpu.VMEM((own, dim), low),
                pltpu.VMEM((own, dim), low),
                pltpu.VMEM((wk.shape[1] // COLS, dim, COLS), low),
                pltpu.VMEM((WO_SLOTS, qc, dim), low),
                pltpu.VMEM((n, own, HEAD), low),
                pltpu.VMEM((n, HEAD, own), low),
                pltpu.VMEM((n, g * own, HEAD), low),
                pltpu.VMEM((n, own, HEAD), low),
                pltpu.VMEM((n, HEAD + ONES, own), low),
                pltpu.VMEM((n, g * own, HEAD), low),
                pltpu.VMEM((n, own, qc), low),
                pltpu.VMEM((n, own, qc), low),
                pltpu.VMEM((own, dim), jnp.float32),
                pltpu.VMEM((8, g * own), jnp.float32),
                pltpu.VMEM((HEAD + ONES, g * own), jnp.float32),
                *[pltpu.VMEM((2 * own, g * own), jnp.float32)] * 2,
                *[pltpu.VMEM((2 * own, g * own), low)] * 2,
                *[pltpu.VMEM((8, g * own), jnp.float32)] * 4,
                *[pltpu.VMEM((own, HEAD), jnp.float32)] * 2,
                pltpu.SemaphoreType.DMA((1,)),
                pltpu.SemaphoreType.DMA((dim // COLS,)),
                pltpu.SemaphoreType.DMA((wk.shape[1] // COLS,)),
                pltpu.SemaphoreType.DMA((WO_SLOTS,)),
                pltpu.SemaphoreType.DMA((4, n)),
                pltpu.SemaphoreType.DMA((4, n)),
            ],
            compiler_params=pltpu.CompilerParams(collective_id=0, has_side_effects=True, vmem_limit_bytes=VMEM),
        )(x, gain.reshape(-1, HEAD), turn.reshape(1, HEAD), wq, wk, wv, wo)
        parts = 4
        return pl.pallas_call(
            functools.partial(_copy, parts),
            out_shape=jax.ShapeDtypeStruct((own, dim), low),
            in_specs=[anywhere],
            out_specs=anywhere,
            scratch_shapes=[pltpu.VMEM((own, dim), low), pltpu.SemaphoreType.DMA((parts,)), pltpu.SemaphoreType.DMA((parts,))],
            compiler_params=pltpu.CompilerParams(vmem_limit_bytes=VMEM),
        )(y)

    tokens, whole = P(("dp", "sp"), None), P(None, None)
    return jax.shard_map(
        step,
        mesh=mesh,
        in_specs=(tokens, P(None), whole, whole, whole, whole),
        out_specs=tokens,
        check_vma=False,
    )
```
